32 devices in a mesh: gx: 8 (over z, y), gy: 4 (over x, core).
Axes of the slice: x: 2, y: 2, z: 4, core: 2. Of those that a mesh axis runs over, the one named last changes fastest.
Arguments:
- state: float32 [4, 2, 4194304], P('gy', None, 'gx'), may hold values from -6 to 6
- fields: float32 [22], replicated, may hold values from 0.5 to 2
- couplings: float32 [22], replicated, may hold values from 0.5 to 2
- noise: float32 [4, 4, 2], P('gy'), may hold values from -5 to 5
Outputs:
- final_state: float32 [4, 2, 4194304], P('gy', None, 'gx')
- record: float32 [4, 2], replicated
The draws below stay inside these ranges and needn't reach their ends.
All inputs are finite; a program needn't handle non-finite values.
Results may differ from the reference program's by a relative error of at most 0.0001.
Values sent between devices are 32-bit elements; how exact they have to be, the bound alone decides.
A program may use at most 128 MiB of HBM per device.

```python
import math
import jax
import jax.numpy as jnp
from jax import lax

NQ = 22
STEPS = 4
TRAJ = 4
DIM = 4194304


def block_levels(rng, dims, pieces, low, top_value):
    loudness, own = 1.0, jax.random.fold_in(rng, 6)
    for dim, blocks in pieces:
        steps = jnp.exp(jax.random.uniform(jax.random.fold_in(own, dim), (blocks,), jnp.float32, low / len(pieces), top_value / len(pieces)))
        loudness = loudness * jnp.repeat(steps, dims[dim] // blocks).reshape([-1 if axis == dim else 1 for axis in range(len(dims))])
    return loudness


def bell_draw(stream_key, shape, scale, limit, shards=(), kind=jnp.bfloat16):
    gain = block_levels(stream_key, shape, shards, -0.22, 0.18) if shards else 1.0
    values = jax.random.normal(stream_key, shape, jnp.float32) * scale * gain
    return jnp.minimum(jnp.maximum(values, -limit), limit).astype(kind)


def setup_inputs(seed: int = 0) -> dict:
    key_of = jax.random.split(jax.random.key(seed), 5)
    return {
        "state": bell_draw(key_of[0], (TRAJ, 2, DIM), 1.0, 6.0, ((0, 4), (2, 8)), jnp.float32),
        "fields": jnp.clip(jnp.exp(jax.random.uniform(key_of[1], (NQ,), jnp.float32, math.log(0.5), math.log(2.0))), 0.5, 2.0),
        "couplings": jnp.clip(jnp.exp(jax.random.uniform(key_of[2], (NQ,), jnp.float32, math.log(0.5), math.log(2.0))), 0.5, 2.0),
        "noise": bell_draw(key_of[3], (TRAJ, STEPS, 2), 1.0, 5.0, ((0, 4),), jnp.float32),
    }


kappa_rate = 4.0
time_step = 0.05

def flip_qubit(amplitudes, qubit):
    shape = amplitudes.shape
    viewed = amplitudes.reshape(shape[0], shape[1], shape[2] >> qubit + 1, 2, 1 << qubit)
    return jnp.flip(viewed, 3).reshape(shape)

def reference(state, fields, couplings, noise):
    dim_total = state.shape[2]
    count_qubits = dim_total.bit_length() - 1
    position = lax.iota(jnp.int32, dim_total)
    spin_list = [1.0 - 2.0 * (position >> q & 1).astype(jnp.float32) for q in range(count_qubits)]
    occupancy = jnp.zeros((dim_total,), jnp.float32)
    energy = jnp.zeros((dim_total,), jnp.float32)
    for q in range(count_qubits):
        occupancy = occupancy + 0.5 * (1.0 - spin_list[q])
        energy = energy + couplings[q] * spin_list[q] * spin_list[(q + 1) % count_qubits]
    occupancy = occupancy / count_qubits
    amplitudes = state
    records = []
    half_root = jnp.sqrt(jnp.float32(time_step / 2.0))
    for step_id in range(noise.shape[1]):
        weight = amplitudes[:, 0] ** 2 + amplitudes[:, 1] ** 2
        norm_sum = lax.optimization_barrier(jnp.sum(weight, axis=1))
        magnet = lax.optimization_barrier(jnp.sum(weight * occupancy[None, :], axis=1)) / norm_sum
        amplitudes = amplitudes * jnp.sqrt(dim_total / norm_sum)[:, None, None]
        flipped = jnp.zeros_like(amplitudes)
        for q in range(count_qubits):
            flipped = flipped + fields[q] * flip_qubit(amplitudes, q)
        hamil = -flipped - energy[None, None, :] * amplitudes
        shift = occupancy[None, :] - magnet[:, None]
        first = (noise[:, step_id, 0] * half_root)[:, None]
        second = (noise[:, step_id, 1] * half_root)[:, None]
        real_part = amplitudes[:, 0]
        imag_part = amplitudes[:, 1]
        damping = time_step * kappa_rate * 0.5 * shift * shift
        kick = jnp.sqrt(jnp.float32(kappa_rate)) * shift
        new_real = real_part + time_step * hamil[:, 1] - damping * real_part + kick * (real_part * first - imag_part * second)
        new_imag = imag_part - time_step * hamil[:, 0] - damping * imag_part + kick * (real_part * second + imag_part * first)
        amplitudes = jnp.stack([new_real, new_imag], axis=1)
        drift = jnp.sqrt(jnp.float32(kappa_rate)) * magnet * time_step
        both = jnp.stack([drift + first[:, 0], drift + second[:, 0]], axis=1)
        records.append(lax.optimization_barrier(jnp.sum(both, axis=0)))
    return (amplitudes, jnp.stack(records))
```

```python
import functools

import jax
import jax.numpy as jnp
from jax import lax
from jax.experimental import pallas as pl
from jax.experimental.pallas import tpu as pltpu
from jax.sharding import PartitionSpec as P

KAPPA = 4.0
DT = 0.05
LANES = 128
LANE_BITS = 7
CHUNK = 128
PIECES = 8
MESH = pl.DeviceIdType.MESH


def ones_in(value):
    return bin(value).count("1")


def bit_of(value, k):
    return lax.rem(lax.div(value, 1 << k), 2)


def flip_bit(value, k):
    return value + (1 - 2 * bit_of(value, k)) * (1 << k)


def flip_bits(value, mask):
    k = 0
    while mask >> k:
        if mask >> k & 1:
            value = flip_bit(value, k)
        k += 1
    return value


def spin(bit):
    return (1 - 2 * bit).astype(jnp.float32)


def wait_bytes(ref, sem):
    pltpu.make_async_copy(ref, ref, sem).wait()


def evolve_kernel(
    bits, paths, steps, spins,
    fields, couplings, noise, state, out, record,
    buf, far, weights, table, outer_energy, outer_ones, edge, sums, marks, kicks,
    own_sem, swap_send, noise_sem, noise_send, arrive, push_send, relay_send,
    far_send, far_recv, sum_send, sum_recv, mark_send, mark_recv, out_sem, out_send, free,
):
    f32 = jnp.float32
    blocks = 1 << bits
    rows = state.shape[0]
    row_bits = rows.bit_length() - 1
    chunk_bits = CHUNK.bit_length() - 1
    chunks = rows // CHUNK
    piece = rows // PIECES
    piece_chunks = piece // CHUNK
    groups = CHUNK // 8

    gx, gy = lax.axis_index("gx"), lax.axis_index("gy")
    high, low = lax.div(gx, blocks), lax.rem(gx, blocks)
    path, core = lax.div(gy, 2), lax.rem(gy, 2)
    home = high == core
    away = high != core
    swap_device = {"gx": core * blocks + low, "gy": path * 2 + high}
    core_device = {"gx": gx, "gy": path * 2 + 1 - core}

    def bit_device(b):
        return {"gx": high * blocks + flip_bit(low, b), "gy": gy}

    def sum_device(o):
        c = 1 - core if o >> bits & 1 else core
        return {"gx": high * blocks + flip_bits(low, o % blocks), "gy": path * 2 + c}

    def mark_device(o):
        h = 1 - high if o & 1 else high
        return {"gx": h * blocks + low, "gy": lax.rem(path + (o >> 1), paths) * 2 + core}

    def remote(src, dst, send, recv, device):
        return pltpu.make_async_remote_copy(
            src_ref=src, dst_ref=dst, send_sem=send, recv_sem=recv, device_id=device, device_id_type=MESH
        )

    def rows_of(p):
        return pl.ds(p * piece, piece)

    @pl.when(home)
    def _():
        for p in range(PIECES):
            pltpu.make_async_copy(state.at[rows_of(p)], buf.at[0, 0, rows_of(p)], own_sem.at[p]).start()
        pltpu.make_async_copy(noise, kicks, noise_sem).start()

    @pl.when(away)
    def _():
        remote(noise, kicks, noise_send, noise_sem, swap_device).start()
        for p in range(PIECES):
            remote(
                state.at[rows_of(p)], buf.at[0, 0, rows_of(p)], swap_send, own_sem.at[p], swap_device
            ).start()

    lane_a = lax.broadcasted_iota(jnp.int32, (LANES, LANES), 0)
    lane_b = lax.broadcasted_iota(jnp.int32, (LANES, LANES), 1)
    distance = lane_a ^ lane_b
    lane_flip = jnp.zeros((LANES, LANES), f32)
    for q in range(LANE_BITS):
        lane_flip = jnp.where(distance == 1 << q, fields[q], lane_flip)
    coarse_flip = lane_flip.astype(jnp.bfloat16)
    fine_flip = (lane_flip - coarse_flip.astype(f32)).astype(jnp.bfloat16)
    weights[:LANES, :LANES] = coarse_flip
    weights[:LANES, LANES:] = fine_flip
    weights[LANES:, :LANES] = coarse_flip
    weights[LANES:, LANES:] = jnp.zeros_like(fine_flip)

    row_ids = lax.broadcasted_iota(jnp.int32, (CHUNK, LANES), 0)
    lane_ids = lax.broadcasted_iota(jnp.int32, (CHUNK, LANES), 1)
    inner_bits = [lane_ids >> q & 1 for q in range(LANE_BITS)]
    inner_bits += [row_ids >> k & 1 for k in range(1, chunk_bits)]
    inner_count = len(inner_bits)
    inner_energy = jnp.zeros((CHUNK, LANES), f32)
    inner_ones = jnp.zeros((CHUNK, LANES), jnp.int32)
    for q in range(inner_count):
        inner_ones = inner_ones + inner_bits[q]
        if q + 1 < inner_count:
            inner_energy = inner_energy + couplings[q] * (spin(inner_bits[q]) * spin(inner_bits[q + 1]))
    table[0] = inner_energy
    table[1] = inner_ones.astype(f32) * (1.0 / spins)

    chunk_qubits = row_bits - chunk_bits
    top_spin = spin(core)
    low_spins = [spin(bit_of(low, b)) for b in range(bits)]

    def fill(k, carry):
        ids = [bit_of(k, t) for t in range(chunk_qubits)]
        z = [spin(b) for b in ids]
        count = ids[0]
        for b in ids[1:]:
            count = count + b
        energy = f32(0.0)
        for t in range(chunk_qubits - 1):
            energy = energy + couplings[inner_count + t] * (z[t] * z[t + 1])
        edge[k] = couplings[inner_count - 1] * z[0]
        for j in range(blocks):
            zb = [low_spins[b] * (-1.0 if j >> b & 1 else 1.0) for b in range(bits)] + [top_spin]
            ones_j = count + core
            for b in range(bits):
                ones_j = ones_j + (1 - bit_of(low, b) if j >> b & 1 else bit_of(low, b))
            e = energy + couplings[spins - 2 - bits] * (z[-1] * zb[0])
            for b in range(bits):
                e = e + couplings[spins - 1 - bits + b] * (zb[b] * zb[b + 1])
            outer_energy[j * chunks + k] = e
            outer_ones[j * chunks + k] = ones_j.astype(f32) * (1.0 / spins)
        return carry

    lax.fori_loop(0, chunks, fill, 0)

    sub = lax.broadcasted_iota(jnp.int32, (8, LANES), 0)
    imag = (sub & 1) == 1
    upper = (sub & 2) == 2
    lane_edge = spin(lax.broadcasted_iota(jnp.int32, (8, LANES), 1) & 1) * (couplings[spins - 1] * top_spin)

    def start_sums(s, norm, tilt):
        sums[s, 0, :8] = norm
        sums[s, 0, 8:] = tilt
        for o in range(1, 2 * blocks):
            remote(
                sums.at[s, 0], sums.at[s, o], sum_send.at[s], sum_recv.at[s], sum_device(o)
            ).start()

    def finish_sums(s):
        others = sums.at[s, pl.ds(1, 2 * blocks - 1)]
        wait_bytes(others, sum_recv.at[s])
        wait_bytes(others, sum_send.at[s])
        total = sums[s, 0]
        for o in range(1, 2 * blocks):
            total = total + sums[s, o]
        norm = jnp.full((8, LANES), jnp.sum(total[:8]), f32)
        tilt = jnp.full((8, LANES), jnp.sum(total[8:]), f32)
        return norm, tilt

    zero = jnp.zeros((8, LANES), f32)

    def first_sums():
        def body(k, carry):
            norm, tilt = carry
            x = buf[0, 0, pl.ds(pl.multiple_of(k * CHUNK, CHUNK), CHUNK), :]
            w = x * x
            ones = table[1] + outer_ones[k]
            norm = norm + jnp.sum(w.reshape(groups, 8, LANES), axis=0)
            tilt = tilt + jnp.sum((w * ones).reshape(groups, 8, LANES), axis=0)
            return norm, tilt

        return lax.fori_loop(0, chunks, body, (zero, zero))

    def step_values(s):
        norm, tilt = finish_sums(s)
        magnet = tilt / norm
        factor = jnp.sqrt(f32(rows * (LANES // 2) * 2 * blocks) / norm)
        half_root = jnp.sqrt(jnp.full((8, LANES), DT / 2.0, f32))
        root_kappa = jnp.sqrt(jnp.full((8, LANES), KAPPA, f32))
        first = kicks[pl.ds(2 * s, 1), :] * half_root
        second = kicks[pl.ds(2 * s + 1, 1), :] * half_root
        drift = root_kappa * magnet * DT
        marks[0, pl.ds(2 * s, 1), :] = (drift + first)[:1]
        marks[0, pl.ds(2 * s + 1, 1), :] = (drift + second)[:1]
        ratio = root_kappa * second * (1.0 / DT)
        damp = factor * (DT * KAPPA * 0.5)
        inner = table[1].reshape(groups, 8, LANES)
        table[2] = (table[0].reshape(groups, 8, LANES) + ratio * inner).reshape(CHUNK, LANES)
        table[3] = (-(damp * inner) * inner).reshape(CHUNK, LANES)
        rate = factor * DT
        return dict(
            magnet=magnet, factor=factor, kick=factor * root_kappa * first, damp=damp, ratio=ratio,
            rate=jnp.where(imag, -rate, rate),
        )

    def update(src, j, begin, end, values, sums_too, carry=None):
        dst = 1 - src

        def body(k, carry):
            base = pl.multiple_of(k * CHUNK, CHUNK)
            here = pl.ds(base, CHUNK)
            x = buf[src, j, here, :]
            coarse = x.astype(jnp.bfloat16)
            fine = (x - coarse.astype(f32)).astype(jnp.bfloat16)
            product = jnp.dot(
                jnp.concatenate([coarse, fine], axis=1), weights[...], preferred_element_type=f32
            )
            total = product[:, :LANES] + product[:, LANES:]
            x3 = x.reshape(groups, 8, LANES)
            near = jnp.where(upper[None], pltpu.roll(x3, 2, 1), pltpu.roll(x3, 6, 1))
            total = total.reshape(groups, 8, LANES) + fields[7] * near + fields[8] * pltpu.roll(x3, 4, 1)
            for t in range(3, chunk_bits):
                size = 1 << (t - 3)
                parts = [x3[(i ^ 1) * size : ((i ^ 1) + 1) * size] for i in range(groups // size)]
                total = total + fields[6 + t] * jnp.concatenate(parts, axis=0)
            for t in range(chunk_bits, row_bits):
                other = pl.multiple_of(flip_bit(k, t - chunk_bits) * CHUNK, CHUNK)
                total = total + fields[6 + t] * buf[src, j, pl.ds(other, CHUNK), :].reshape(groups, 8, LANES)
            for b in range(bits):
                total = total + fields[6 + row_bits + b] * buf[src, j ^ 1 << b, here, :].reshape(groups, 8, LANES)
            total = total + fields[spins - 1] * far[j, here, :].reshape(groups, 8, LANES)

            ones = outer_ones[j * chunks + k]
            shift = ones - values["magnet"]
            constant = values["factor"] + shift * (values["kick"] - values["damp"] * shift)
            slope = values["kick"] - 2.0 * (values["damp"] * shift)
            level = lane_edge + outer_energy[j * chunks + k] + values["ratio"] * shift
            inner = table[1].reshape(groups, 8, LANES)
            side = jnp.concatenate(
                [jnp.broadcast_to((level + edge[k])[None], (groups // 2, 8, LANES)),
                 jnp.broadcast_to((level - edge[k])[None], (groups // 2, 8, LANES))], axis=0
            )
            diagonal = table[2].reshape(groups, 8, LANES) + side
            turned = values["rate"] * (total + x3 * diagonal)
            turned = jnp.where(imag[None], pltpu.roll(turned, 1, 1), pltpu.roll(turned, 7, 1))
            keep = table[3].reshape(groups, 8, LANES) + constant + slope * inner
            new = keep * x3 + turned
            buf[dst, j, here, :] = new.reshape(CHUNK, LANES)
            if not sums_too:
                return carry
            norm, tilt = carry
            w = new * new
            some = jnp.sum(w, axis=0)
            return norm + some, tilt + jnp.sum(w * inner, axis=0) + ones * some

        if not sums_too:
            lax.fori_loop(begin, end, body, 0)
            return None
        return lax.fori_loop(begin, end, body, carry or (zero, zero))

    def send_far(src, j, where=None):
        where = pl.ds(0, rows) if where is None else where
        remote(
            buf.at[src, j, where], far.at[j, where], far_send.at[j], far_recv.at[j], core_device
        ).start()

    order = sorted(range(blocks), key=lambda j: (ones_in(j), j))
    levels = [[j for j in order if ones_in(j) == n] for n in range(bits + 1)]

    def last_hop(j, p):
        on = [b for b in range(bits) if j >> b & 1]
        return on[-1] if p % 4 == 3 else on[(p // 4) % (len(on) - 1)]

    def arrived(j, p):
        wait_bytes(buf.at[0, j, rows_of(p)], arrive.at[j, p])
        send_far(0, j, rows_of(p))
        for b in range(bits):
            target = j | 1 << b
            if not j >> b & 1 and last_hop(target, p) == b:
                remote(
                    buf.at[0, j, rows_of(p)], buf.at[0, target, rows_of(p)],
                    relay_send.at[target], arrive.at[target, p], bit_device(b),
                ).start()

    lag = 2
    for p in range(PIECES):
        wait_bytes(buf.at[0, 0, rows_of(p)], own_sem.at[p])
        for b in range(bits):
            remote(
                buf.at[0, 0, rows_of(p)], buf.at[0, 1 << b, rows_of(p)],
                push_send.at[b], arrive.at[1 << b, p], bit_device(b),
            ).start()
        send_far(0, 0, rows_of(p))
        if p >= lag:
            for j in levels[1]:
                arrived(j, p - lag)
    start_sums(0, *first_sums())
    for p in range(PIECES - lag, PIECES):
        for j in levels[1]:
            arrived(j, p)
    wait_bytes(kicks, noise_sem)

    values = step_values(0)
    everything = pl.ds(0, rows)

    def far_ready(j):
        wait_bytes(far.at[j, everything], far_recv.at[j])

    def whole(src, j, sums_too):
        far_ready(j)
        return update(src, j, 0, chunks, values, sums_too)

    sums_next = None
    for n in range(2, bits + 1):
        for j in levels[n - 2]:
            got = whole(0, j, j == 0)
            if j == 0:
                start_sums(1, *got)
        if n < bits:
            for p in range(PIECES):
                for j in levels[n]:
                    arrived(j, p)
    for j in levels[bits - 1]:
        far_ready(j)
    got = (zero, zero)
    last = levels[bits][0]
    for p in range(PIECES):
        arrived(last, p)
        for j in levels[bits - 1]:
            part = update(0, j, p * piece_chunks, (p + 1) * piece_chunks, values, j == 0, got)
            if j == 0:
                got = part
    if bits == 1:
        start_sums(1, *got)
    whole(0, last, False)

    @pl.when(away)
    def _():
        wait_bytes(state, swap_send)
        wait_bytes(noise, noise_send)

    for b in range(bits):
        wait_bytes(buf.at[0, 0], push_send.at[b])
    for j in order:
        if ones_in(j) >= 2:
            wait_bytes(buf.at[0, j], relay_send.at[j])

    in_flight = set(order)

    def send_next(src, j):
        pl.semaphore_wait(free.at[j], 1)
        wait_bytes(buf.at[src, j], far_send.at[j])
        send_far(src, j)

    def needed(s):
        return [j for j in order if ones_in(j) <= steps - 1 - s]

    for j in needed(1):
        pl.semaphore_signal(free.at[j], 1, device_id=core_device, device_id_type=MESH)
    for j in needed(1):
        send_next(1, j)

    for s in range(1, steps - 1):
        src = s % 2
        values = step_values(s)
        waiting = None
        for j in needed(s):
            got = whole(src, j, j == 0)
            if j == 0:
                start_sums(s + 1, *got)
            if j in needed(s + 1):
                pl.semaphore_signal(free.at[j], 1, device_id=core_device, device_id_type=MESH)
            if waiting is not None:
                send_next(1 - src, waiting)
            waiting = j if j in needed(s + 1) else None
        if waiting is not None:
            send_next(1 - src, waiting)

    src = (steps - 1) % 2
    values = step_values(steps - 1)
    for o in range(1, 2 * paths):
        remote(marks.at[0], marks.at[o], mark_send, mark_recv, mark_device(o)).start()
    far_ready(0)

    def deliver(p):
        @pl.when(home)
        def _():
            pltpu.make_async_copy(buf.at[1 - src, 0, rows_of(p)], out.at[rows_of(p)], out_sem).start()

        @pl.when(away)
        def _():
            remote(
                buf.at[1 - src, 0, rows_of(p)], out.at[rows_of(p)], out_send, out_sem, swap_device
            ).start()

    for p in range(PIECES):
        update(src, 0, p * piece_chunks, (p + 1) * piece_chunks, values, False)
        if p:
            deliver(p - 1)
    deliver(PIECES - 1)

    others = marks.at[pl.ds(1, 2 * paths - 1)]
    wait_bytes(others, mark_recv)
    wait_bytes(others, mark_send)
    total = marks[0]
    for o in range(1, 2 * paths):
        total = total + marks[o]
    record[...] = total
    for j in order:
        wait_bytes(buf.at[0, j], far_send.at[j])
    wait_bytes(out, out_sem)

    @pl.when(away)
    def _():
        wait_bytes(out, out_send)


def shards(state, fields, couplings, noise):
    local_len = state.shape[2]
    steps = noise.shape[1]
    bits = lax.axis_size("gx").bit_length() - 2
    paths = lax.axis_size("gy") // 2
    spins = local_len.bit_length() - 1 + bits + 1
    blocks = 1 << bits
    rows = 2 * local_len // LANES
    chunks = rows // CHUNK
    f32 = jnp.float32
    mixed = state.reshape(2, rows // 2, LANES).transpose(1, 0, 2).reshape(rows, LANES)
    kicks = jnp.broadcast_to(noise.reshape(steps * 2, 1), (steps * 2, LANES))
    smem = pl.BlockSpec(memory_space=pltpu.SMEM)
    hbm = pl.BlockSpec(memory_space=pl.ANY)
    dma, regular = pltpu.SemaphoreType.DMA, pltpu.SemaphoreType.REGULAR
    tile = (steps * 2, LANES)
    out, record = pl.pallas_call(
        functools.partial(evolve_kernel, bits, paths, steps, spins),
        in_specs=[smem, smem, hbm, hbm],
        out_specs=[hbm, pl.BlockSpec(memory_space=pltpu.VMEM)],
        out_shape=[jax.ShapeDtypeStruct((rows, LANES), f32), jax.ShapeDtypeStruct(tile, f32)],
        scratch_shapes=[
            pltpu.VMEM((2, blocks, rows, LANES), f32),
            pltpu.VMEM((blocks, rows, LANES), f32),
            pltpu.VMEM((2 * LANES, 2 * LANES), jnp.bfloat16),
            pltpu.VMEM((4, CHUNK, LANES), f32),
            pltpu.SMEM((blocks * chunks,), f32),
            pltpu.SMEM((blocks * chunks,), f32),
            pltpu.SMEM((chunks,), f32),
            pltpu.VMEM((steps, 2 * blocks, 16, LANES), f32),
            pltpu.VMEM((2 * paths,) + tile, f32),
            pltpu.VMEM(tile, f32),
            dma((PIECES,)), dma, dma, dma, dma((blocks, PIECES)), dma((bits,)), dma((blocks,)),
            dma((blocks,)), dma((blocks,)), dma((steps,)), dma((steps,)), dma, dma, dma, dma,
            regular((blocks,)),
        ],
        compiler_params=pltpu.CompilerParams(has_side_effects=True, vmem_limit_bytes=60 << 20),
    )(fields, couplings, kicks, mixed)
    final = out.reshape(rows // 2, 2, LANES).transpose(1, 0, 2).reshape(1, 2, local_len)
    return final, record[:, 0].reshape(steps, 2)


def solution(mesh):
    placed = (P("gy", None, "gx"), P(), P(), P("gy", None, None))
    return jax.shard_map(
        shards, mesh=mesh, in_specs=placed, out_specs=(P("gy", None, "gx"), P()), check_vma=False
    )
```

```python
import functools

import jax
import jax.numpy as jnp
from jax import lax
from jax.experimental import pallas as pl
from jax.experimental.pallas import tpu as pltpu
from jax.sharding import PartitionSpec as P

KAPPA = 4.0
DT = 0.05
LANES = 128
LANE_BITS = 7
SIDE = 256
SIDE_BITS = 8
CHUNK = 2 * SIDE
PART = 64
PIECES = 8
MESH = pl.DeviceIdType.MESH


def ones_in(value):
    return bin(value).count("1")


def bit_of(value, k):
    return lax.rem(lax.div(value, 1 << k), 2)


def flip_bit(value, k):
    return value + (1 - 2 * bit_of(value, k)) * (1 << k)


def flip_bits(value, mask):
    k = 0
    while mask >> k:
        if mask >> k & 1:
            value = flip_bit(value, k)
        k += 1
    return value


def other_block(j, b):
    return j ^ 1 << b if isinstance(j, int) else flip_bit(j, b)


def spin(bit):
    return (1 - 2 * bit).astype(jnp.float32)


def wait_bytes(ref, sem):
    pltpu.make_async_copy(ref, ref, sem).wait()


def evolve_kernel(
    bits, paths, steps, spins,
    fields, couplings, noise, state, out, record,
    even, odd, far, row_flips, pair_flips, ahead, later, table, outer_energy, outer_ones, edge, sums, marks, kicks,
    own_sem, swap_send, noise_sem, noise_send, arrive, push_send, relay_send,
    far_send, far_recv, sum_send, sum_recv, mark_send, mark_recv, out_sem, out_send, free,
):
    f32 = jnp.float32
    blocks = 1 << bits
    rows = state.shape[0]
    row_bits = rows.bit_length() - 1
    chunk_bits = CHUNK.bit_length() - 1
    bufs = (even, odd)
    chunks = rows // CHUNK
    piece = rows // PIECES
    piece_chunks = piece // CHUNK
    groups = SIDE // 8
    part_groups = PART // 8

    gx, gy = lax.axis_index("gx"), lax.axis_index("gy")
    high, low = lax.div(gx, blocks), lax.rem(gx, blocks)
    path, core = lax.div(gy, 2), lax.rem(gy, 2)
    home = high == core
    away = high != core
    swap_device = {"gx": core * blocks + low, "gy": path * 2 + high}
    core_device = {"gx": gx, "gy": path * 2 + 1 - core}

    def bit_device(b):
        return {"gx": high * blocks + flip_bit(low, b), "gy": gy}

    def sum_device(o):
        c = 1 - core if o >> bits & 1 else core
        return {"gx": high * blocks + flip_bits(low, o % blocks), "gy": path * 2 + c}

    def mark_device(o):
        h = 1 - high if o & 1 else high
        return {"gx": h * blocks + low, "gy": lax.rem(path + (o >> 1), paths) * 2 + core}

    def remote(src, dst, send, recv, device):
        return pltpu.make_async_remote_copy(
            src_ref=src, dst_ref=dst, send_sem=send, recv_sem=recv, device_id=device, device_id_type=MESH
        )

    def rows_of(p):
        return pl.ds(p * piece if isinstance(p, int) else pl.multiple_of(p * piece, piece), piece)

    @pl.when(home)
    def _():
        for p in range(PIECES):
            pltpu.make_async_copy(state.at[rows_of(p)], even.at[0, rows_of(p)], own_sem.at[p]).start()
        pltpu.make_async_copy(noise, kicks, noise_sem).start()

    @pl.when(away)
    def _():
        remote(noise, kicks, noise_send, noise_sem, swap_device).start()
        for p in range(PIECES):
            remote(
                state.at[rows_of(p)], even.at[0, rows_of(p)], swap_send, own_sem.at[p], swap_device
            ).start()

    place_a = lax.broadcasted_iota(jnp.int32, (SIDE, SIDE), 0)
    place_b = lax.broadcasted_iota(jnp.int32, (SIDE, SIDE), 1)
    distance = place_a ^ place_b
    flips = jnp.zeros((SIDE, SIDE), f32)
    for k in range(1, SIDE_BITS):
        flips = jnp.where(distance == 1 << k, fields[6 + k], flips)
    row_flips[0] = flips.astype(jnp.bfloat16)
    row_flips[1] = (flips - flips.astype(jnp.bfloat16).astype(f32)).astype(jnp.bfloat16)
    flips = jnp.where(distance == LANES, fields[6 + SIDE_BITS], jnp.zeros((SIDE, SIDE), f32))
    for q in range(LANE_BITS):
        flips = jnp.where(distance == 1 << q, fields[q], flips)
    pair_flips[0] = flips.astype(jnp.bfloat16)
    pair_flips[1] = (flips - flips.astype(jnp.bfloat16).astype(f32)).astype(jnp.bfloat16)

    row_ids = lax.broadcasted_iota(jnp.int32, (SIDE, LANES), 0)
    lane_ids = lax.broadcasted_iota(jnp.int32, (SIDE, LANES), 1)
    inner_bits = [lane_ids >> q & 1 for q in range(LANE_BITS)]
    inner_bits += [row_ids >> k & 1 for k in range(1, SIDE_BITS)]
    inner_count = len(inner_bits)
    inner_energy = jnp.zeros((SIDE, LANES), f32)
    inner_ones = jnp.zeros((SIDE, LANES), jnp.int32)
    for q in range(inner_count):
        inner_ones = inner_ones + inner_bits[q]
        if q + 1 < inner_count:
            inner_energy = inner_energy + couplings[q] * (spin(inner_bits[q]) * spin(inner_bits[q + 1]))
    table[0] = inner_energy
    table[1] = inner_ones.astype(f32) * (1.0 / spins)

    chunk_qubits = row_bits - chunk_bits
    top_spin = spin(core)
    low_spins = [spin(bit_of(low, b)) for b in range(bits)]

    def fill(k, carry):
        ids = [bit_of(k, t) for t in range(chunk_qubits)]
        z = [spin(b) for b in ids]
        count = ids[0]
        for b in ids[1:]:
            count = count + b
        energy = f32(0.0)
        for t in range(chunk_qubits - 1):
            energy = energy + couplings[inner_count + 1 + t] * (z[t] * z[t + 1])
        edge[k] = couplings[inner_count] * z[0]
        for j in range(blocks):
            zb = [low_spins[b] * (-1.0 if j >> b & 1 else 1.0) for b in range(bits)] + [top_spin]
            ones_j = count + core
            for b in range(bits):
                ones_j = ones_j + (1 - bit_of(low, b) if j >> b & 1 else bit_of(low, b))
            e = energy + couplings[spins - 2 - bits] * (z[-1] * zb[0])
            for b in range(bits):
                e = e + couplings[spins - 1 - bits + b] * (zb[b] * zb[b + 1])
            outer_energy[j * chunks + k] = e
            outer_ones[j * chunks + k] = ones_j.astype(f32) * (1.0 / spins)
        return carry

    lax.fori_loop(0, chunks, fill, 0)

    sub = lax.broadcasted_iota(jnp.int32, (8, LANES), 0)
    imag = (sub & 1) == 1
    lane_edge = spin(lax.broadcasted_iota(jnp.int32, (8, LANES), 1) & 1) * (couplings[spins - 1] * top_spin)

    def start_sums(s, norm, tilt):
        sums[s, 0, :8] = norm
        sums[s, 0, 8:] = tilt
        for o in range(1, 2 * blocks):
            remote(
                sums.at[s, 0], sums.at[s, o], sum_send.at[s], sum_recv.at[s], sum_device(o)
            ).start()

    def finish_sums(s):
        others = sums.at[s, pl.ds(1, 2 * blocks - 1)]
        wait_bytes(others, sum_recv.at[s])
        wait_bytes(others, sum_send.at[s])
        total = sums[s, 0]
        for o in range(1, 2 * blocks):
            total = total + sums[s, o]
        norm = jnp.full((8, LANES), jnp.sum(total[:8]), f32)
        tilt = jnp.full((8, LANES), jnp.sum(total[8:]), f32)
        return norm, tilt

    zero = jnp.zeros((8, LANES), f32)

    def first_sums():
        def body(k, carry):
            norm, tilt = carry
            for side in range(2):
                base = pl.multiple_of(k * CHUNK + side * SIDE, SIDE)
                x = even[0, pl.ds(base, SIDE), :]
                w = x * x
                ones = table[1] + (outer_ones[k] + side / spins)
                norm = norm + jnp.sum(w.reshape(groups, 8, LANES), axis=0)
                tilt = tilt + jnp.sum((w * ones).reshape(groups, 8, LANES), axis=0)
            return norm, tilt

        return lax.fori_loop(0, chunks, body, (zero, zero))

    def step_values(s):
        norm, tilt = finish_sums(s)
        magnet = tilt / norm
        factor = jnp.sqrt(f32(rows * (LANES // 2) * 2 * blocks) / norm)
        half_root = jnp.sqrt(jnp.full((8, LANES), DT / 2.0, f32))
        root_kappa = jnp.sqrt(jnp.full((8, LANES), KAPPA, f32))
        first = kicks[pl.ds(2 * s, 1), :] * half_root
        second = kicks[pl.ds(2 * s + 1, 1), :] * half_root
        drift = root_kappa * magnet * DT
        marks[0, pl.ds(2 * s, 1), :] = (drift + first)[:1]
        marks[0, pl.ds(2 * s + 1, 1), :] = (drift + second)[:1]
        ratio = root_kappa * second * (1.0 / DT)
        damp = factor * (DT * KAPPA * 0.5)
        table[2] = table[0] + (ratio.reshape(1, 8, LANES) * table[1].reshape(groups, 8, LANES)).reshape(SIDE, LANES)
        rate = factor * DT
        return dict(
            magnet=magnet, factor=factor, kick=factor * root_kappa * first, damp=damp, ratio=ratio,
            rate=jnp.where(imag, -rate, rate),
        )

    def flip_tile(src, j, k):
        x = jnp.concatenate(
            [bufs[src][j, pl.ds(pl.multiple_of(k * CHUNK + side * SIDE, SIDE), SIDE), :] for side in range(2)],
            axis=1,
        )
        coarse = x.astype(jnp.bfloat16)
        fine = (x - coarse.astype(f32)).astype(jnp.bfloat16)
        left = jnp.concatenate([row_flips[0], row_flips[0], row_flips[1], coarse, fine, coarse], axis=1)
        right = jnp.concatenate([coarse, fine, coarse, pair_flips[0], pair_flips[0], pair_flips[1]], axis=0)
        return jnp.dot(left, right, preferred_element_type=f32)

    base_ones = table[1, :8]

    def finish(src, j, k, tile, values, carry):
        here, there = bufs[src], bufs[1 - src]
        ones = outer_ones[j * chunks + k]
        keeps = []
        for n in range(SIDE_BITS - 1):
            shift = base_ones + (ones + n / spins - values["magnet"])
            keeps.append(values["factor"] + shift * (values["kick"] - values["damp"] * shift))
        level = lane_edge + outer_energy[j * chunks + k]
        weights = [None] * (SIDE_BITS - 1)
        for side in range(2):
            shift = ones + side / spins - values["magnet"]
            base_level = level + values["ratio"] * shift + (-edge[k] if side else edge[k])
            link = -couplings[inner_count - 1] if side else couplings[inner_count - 1]
            for part in range(SIDE // PART):
                offset = k * CHUNK + side * SIDE + part * PART
                rows_here = pl.ds(pl.multiple_of(offset, PART), PART)
                x = here[j, rows_here, :]
                total = tile[part * PART : (part + 1) * PART, side * LANES : (side + 1) * LANES]
                for t in range(chunk_bits, row_bits):
                    moved = flip_bit(k, t - chunk_bits) * CHUNK + side * SIDE + part * PART
                    total = total + fields[6 + t] * here[j, pl.ds(pl.multiple_of(moved, PART), PART), :]
                for b in range(bits):
                    total = total + fields[6 + row_bits + b] * here[other_block(j, b), rows_here, :]
                total = total + fields[spins - 1] * far[j, rows_here, :]
                top = part * PART * 2 // SIDE
                side_level = base_level - link if top else base_level + link
                x3 = x.reshape(part_groups, 8, LANES)
                diagonal = table[2, part * PART : (part + 1) * PART].reshape(part_groups, 8, LANES) + side_level[None]
                turned = values["rate"] * (total.reshape(part_groups, 8, LANES) + x3 * diagonal)
                turned = jnp.where(imag[None], pltpu.roll(turned, 1, 1), pltpu.roll(turned, 7, 1))
                counts = [ones_in(part * part_groups + g) + side for g in range(part_groups)]
                keep = jnp.concatenate([keeps[n][None] for n in counts], axis=0)
                new = keep * x3 + turned
                there[j, rows_here, :] = new.reshape(PART, LANES)
                if carry is not None:
                    w = new * new
                    for g, n in enumerate(counts):
                        weights[n] = w[g] if weights[n] is None else weights[n] + w[g]
        if carry is None:
            return None
        norm, tilt = carry
        some, scaled = weights[0], None
        for n in range(1, SIDE_BITS - 1):
            some = some + weights[n]
            scaled = weights[n] * (n / spins) if scaled is None else scaled + weights[n] * (n / spins)
        return norm + some, tilt + scaled + (base_ones + ones) * some

    def update(src, j, begin, end, values, sums_too, carry=None):
        ahead[...] = flip_tile(src, j, begin)

        def body(m, carry):
            k = begin + 2 * m
            later[...] = flip_tile(src, j, k + 1)
            carry = finish(src, j, k, ahead, values, carry)
            ahead[...] = flip_tile(src, j, jnp.minimum(k + 2, end - 1))
            return finish(src, j, k + 1, later, values, carry)

        trips = lax.div(end - begin, 2)
        if not sums_too:
            def plain(m, nothing):
                body(m, None)
                return nothing

            lax.fori_loop(0, trips, plain, 0)
            return None
        return lax.fori_loop(0, trips, body, carry or (zero, zero))

    def send_far(src, j, where=None):
        where = pl.ds(0, rows) if where is None else where
        remote(
            bufs[src].at[j, where], far.at[j, where], far_send.at[j], far_recv.at[j], core_device
        ).start()

    order = sorted(range(blocks), key=lambda j: (ones_in(j), j))
    levels = [[j for j in order if ones_in(j) == n] for n in range(bits + 1)]

    def last_hop(j, p):
        on = [b for b in range(bits) if j >> b & 1]
        return on[-1] if p % 4 == 3 else on[(p // 4) % (len(on) - 1)]

    def arrived(j, p):
        wait_bytes(even.at[j, rows_of(p)], arrive.at[j, p])
        send_far(0, j, rows_of(p))
        for b in range(bits):
            target = j | 1 << b
            if not j >> b & 1 and last_hop(target, p) == b:
                remote(
                    even.at[j, rows_of(p)], even.at[target, rows_of(p)],
                    relay_send.at[target], arrive.at[target, p], bit_device(b),
                ).start()

    lag = 2
    for p in range(PIECES):
        wait_bytes(even.at[0, rows_of(p)], own_sem.at[p])
        for b in range(bits):
            remote(
                even.at[0, rows_of(p)], even.at[1 << b, rows_of(p)],
                push_send.at[b], arrive.at[1 << b, p], bit_device(b),
            ).start()
        send_far(0, 0, rows_of(p))
        if p >= lag:
            for j in levels[1]:
                arrived(j, p - lag)
    start_sums(0, *first_sums())
    for p in range(PIECES - lag, PIECES):
        for j in levels[1]:
            arrived(j, p)
    wait_bytes(kicks, noise_sem)

    values = step_values(0)
    everything = pl.ds(0, rows)

    def far_ready(j):
        wait_bytes(far.at[j, everything], far_recv.at[j])

    def whole(src, j, sums_too):
        far_ready(j)
        return update(src, j, 0, chunks, values, sums_too)

    for n in range(2, bits + 1):
        for j in levels[n - 2]:
            got = whole(0, j, j == 0)
            if j == 0:
                start_sums(1, *got)
        if n < bits:
            for p in range(PIECES):
                for j in levels[n]:
                    arrived(j, p)
    last = blocks - 1

    def late_block(t, carry):
        final = t == 2 * bits
        half = lax.div(t, bits)

        @pl.when((lax.rem(t, bits) == 0) & (t < 2 * bits))
        def _():
            def take(p, nothing):
                arrived(last, half * (PIECES // 2) + p)
                return nothing

            lax.fori_loop(0, PIECES // 2, take, 0)

        j = last - jnp.where(final, 0, lax.shift_left(1, lax.rem(t, bits)))

        @pl.when((t < bits) | final)
        def _():
            far_ready(j)

        begin = jnp.where(final, 0, half * (chunks // 2))
        end = jnp.where(final, chunks, (half + 1) * (chunks // 2))
        update(0, j, begin, end, values, False)
        return carry

    lax.fori_loop(0, 2 * bits + 1, late_block, 0)

    @pl.when(away)
    def _():
        wait_bytes(state, swap_send)
        wait_bytes(noise, noise_send)

    for b in range(bits):
        wait_bytes(even.at[0], push_send.at[b])
    for j in order:
        if ones_in(j) >= 2:
            wait_bytes(even.at[j], relay_send.at[j])

    def send_next(src, j):
        pl.semaphore_wait(free.at[j], 1)
        wait_bytes(bufs[src].at[j], far_send.at[j])
        send_far(src, j)

    def release(j):
        pl.semaphore_signal(free.at[j], 1, device_id=core_device, device_id_type=MESH)

    def needed(s):
        return [j for j in range(blocks) if ones_in(j) <= steps - 1 - s]

    def is_needed(j, s):
        count = bit_of(j, 0)
        for b in range(1, bits):
            count = count + bit_of(j, b)
        return count <= steps - 1 - s

    for j in needed(1):
        release(j)
    for j in needed(1):
        send_next(1, j)

    for s in range(1, steps - 1):
        src = s % 2
        values = step_values(s)
        start_sums(s + 1, *whole(src, 0, True))
        release(0)
        previous = 0
        rest = needed(s)[1:]
        while rest:
            first = stop = rest[0]
            while stop in rest:
                stop += 1
            rest = [j for j in rest if j >= stop]

            def one_block(j, carry, first=first, previous=previous, src=src, s=s, values=values):
                far_ready(j)
                update(src, j, 0, chunks, values, False)

                @pl.when(is_needed(j, s + 1))
                def _():
                    release(j)

                before = jnp.where(j == first, previous, j - 1)

                @pl.when(is_needed(before, s + 1))
                def _():
                    send_next(1 - src, before)

                return carry

            lax.fori_loop(first, stop, one_block, 0)
            previous = stop - 1
        if previous in needed(s + 1):
            send_next(1 - src, previous)

    src = (steps - 1) % 2
    values = step_values(steps - 1)
    for o in range(1, 2 * paths):
        remote(marks.at[0], marks.at[o], mark_send, mark_recv, mark_device(o)).start()
    far_ready(0)

    def deliver(p):
        @pl.when(home)
        def _():
            pltpu.make_async_copy(bufs[1 - src].at[0, rows_of(p)], out.at[rows_of(p)], out_sem).start()

        @pl.when(away)
        def _():
            remote(
                bufs[1 - src].at[0, rows_of(p)], out.at[rows_of(p)], out_send, out_sem, swap_device
            ).start()

    def last_piece(p, carry):
        update(src, 0, p * piece_chunks, (p + 1) * piece_chunks, values, False)

        @pl.when(p > 0)
        def _():
            deliver(p - 1)

        return carry

    lax.fori_loop(0, PIECES, last_piece, 0)
    deliver(PIECES - 1)

    others = marks.at[pl.ds(1, 2 * paths - 1)]
    wait_bytes(others, mark_recv)
    wait_bytes(others, mark_send)
    total = marks[0]
    for o in range(1, 2 * paths):
        total = total + marks[o]
    record[...] = total
    for j in order:
        wait_bytes(even.at[j], far_send.at[j])
    wait_bytes(out, out_sem)

    @pl.when(away)
    def _():
        wait_bytes(out, out_send)


def shards(state, fields, couplings, noise):
    local_len = state.shape[2]
    steps = noise.shape[1]
    bits = lax.axis_size("gx").bit_length() - 2
    paths = lax.axis_size("gy") // 2
    spins = local_len.bit_length() - 1 + bits + 1
    blocks = 1 << bits
    rows = 2 * local_len // LANES
    chunks = rows // CHUNK
    f32 = jnp.float32
    mixed = state.reshape(2, rows // 2, LANES).transpose(1, 0, 2).reshape(rows, LANES)
    kicks = jnp.broadcast_to(noise.reshape(steps * 2, 1), (steps * 2, LANES))
    smem = pl.BlockSpec(memory_space=pltpu.SMEM)
    hbm = pl.BlockSpec(memory_space=pl.ANY)
    dma, regular = pltpu.SemaphoreType.DMA, pltpu.SemaphoreType.REGULAR
    tile = (steps * 2, LANES)
    out, record = pl.pallas_call(
        functools.partial(evolve_kernel, bits, paths, steps, spins),
        in_specs=[smem, smem, hbm, hbm],
        out_specs=[hbm, pl.BlockSpec(memory_space=pltpu.VMEM)],
        out_shape=[jax.ShapeDtypeStruct((rows, LANES), f32), jax.ShapeDtypeStruct(tile, f32)],
        scratch_shapes=[
            pltpu.VMEM((blocks, rows, LANES), f32),
            pltpu.VMEM((blocks, rows, LANES), f32),
            pltpu.VMEM((blocks, rows, LANES), f32),
            pltpu.VMEM((2, SIDE, SIDE), jnp.bfloat16),
            pltpu.VMEM((2, SIDE, SIDE), jnp.bfloat16),
            pltpu.VMEM((SIDE, SIDE), f32),
            pltpu.VMEM((SIDE, SIDE), f32),
            pltpu.VMEM((3, SIDE, LANES), f32),
            pltpu.SMEM((blocks * chunks,), f32),
            pltpu.SMEM((blocks * chunks,), f32),
            pltpu.SMEM((chunks,), f32),
            pltpu.VMEM((steps, 2 * blocks, 16, LANES), f32),
            pltpu.VMEM((2 * paths,) + tile, f32),
            pltpu.VMEM(tile, f32),
            dma((PIECES,)), dma, dma, dma, dma((blocks, PIECES)), dma((bits,)), dma((blocks,)),
            dma((blocks,)), dma((blocks,)), dma((steps,)), dma((steps,)), dma, dma, dma, dma,
            regular((blocks,)),
        ],
        compiler_params=pltpu.CompilerParams(has_side_effects=True, vmem_limit_bytes=60 << 20),
    )(fields, couplings, kicks, mixed)
    final = out.reshape(rows // 2, 2, LANES).transpose(1, 0, 2).reshape(1, 2, local_len)
    return final, record[:, 0].reshape(steps, 2)


def solution(mesh):
    placed = (P("gy", None, "gx"), P(), P(), P("gy", None, None))
    return jax.shard_map(
        shards, mesh=mesh, in_specs=placed, out_specs=(P("gy", None, "gx"), P()), check_vma=False
    )
```

```python
import functools

import jax
import jax.numpy as jnp
from jax import lax
from jax.experimental import pallas as pl
from jax.experimental.pallas import tpu as pltpu
from jax.sharding import PartitionSpec as P

KAPPA = 4.0
DT = 0.05
LANES = 128
LANE_BITS = 7
SIDE = 256
SIDE_BITS = 8
CHUNK = 2 * SIDE
PART = 64
PIECES = 8
MESH = pl.DeviceIdType.MESH


def ones_in(value):
    return bin(value).count("1")


def bit_of(value, k):
    return lax.rem(lax.div(value, 1 << k), 2)


def flip_bit(value, k):
    return value + (1 - 2 * bit_of(value, k)) * (1 << k)


def flip_bits(value, mask):
    k = 0
    while mask >> k:
        if mask >> k & 1:
            value = flip_bit(value, k)
        k += 1
    return value


def other_block(j, b):
    return j ^ 1 << b if isinstance(j, int) else flip_bit(j, b)


def spin(bit):
    return (1 - 2 * bit).astype(jnp.float32)


def wait_bytes(ref, sem):
    pltpu.make_async_copy(ref, ref, sem).wait()


def evolve_kernel(
    bits, paths, steps, spins,
    fields, couplings, noise, state, out, record,
    even, odd, far, row_flips, pair_flips, ahead, later, table, outer_energy, outer_ones, edge, sums, marks, kicks,
    own_sem, swap_send, noise_sem, noise_send, arrive, push_send, relay_send,
    far_send, far_recv, sum_send, sum_recv, mark_send, mark_recv, out_sem, out_send, free,
):
    f32 = jnp.float32
    blocks = 1 << bits
    rows = state.shape[0]
    row_bits = rows.bit_length() - 1
    chunk_bits = CHUNK.bit_length() - 1
    bufs = (even, odd)
    chunks = rows // CHUNK
    piece = rows // PIECES
    piece_chunks = piece // CHUNK
    groups = SIDE // 8
    part_groups = PART // 8

    gx, gy = lax.axis_index("gx"), lax.axis_index("gy")
    high, low = lax.div(gx, blocks), lax.rem(gx, blocks)
    path, core = lax.div(gy, 2), lax.rem(gy, 2)
    home = high == core
    away = high != core
    swap_device = {"gx": core * blocks + low, "gy": path * 2 + high}
    core_device = {"gx": gx, "gy": path * 2 + 1 - core}

    def bit_device(b):
        return {"gx": high * blocks + flip_bit(low, b), "gy": gy}

    def sum_device(o):
        c = 1 - core if o >> bits & 1 else core
        return {"gx": high * blocks + flip_bits(low, o % blocks), "gy": path * 2 + c}

    def mark_device(o):
        h = 1 - high if o & 1 else high
        return {"gx": h * blocks + low, "gy": lax.rem(path + (o >> 1), paths) * 2 + core}

    def remote(src, dst, send, recv, device):
        return pltpu.make_async_remote_copy(
            src_ref=src, dst_ref=dst, send_sem=send, recv_sem=recv, device_id=device, device_id_type=MESH
        )

    def rows_of(p):
        return pl.ds(p * piece if isinstance(p, int) else pl.multiple_of(p * piece, piece), piece)

    @pl.when(home)
    def _():
        for p in range(PIECES):
            pltpu.make_async_copy(state.at[rows_of(p)], even.at[0, rows_of(p)], own_sem.at[p]).start()
        pltpu.make_async_copy(noise, kicks, noise_sem).start()

    @pl.when(away)
    def _():
        remote(noise, kicks, noise_send, noise_sem, swap_device).start()
        for p in range(PIECES):
            remote(
                state.at[rows_of(p)], even.at[0, rows_of(p)], swap_send, own_sem.at[p], swap_device
            ).start()

    place_a = lax.broadcasted_iota(jnp.int32, (SIDE, SIDE), 0)
    place_b = lax.broadcasted_iota(jnp.int32, (SIDE, SIDE), 1)
    distance = place_a ^ place_b
    flips = jnp.zeros((SIDE, SIDE), f32)
    for k in range(1, SIDE_BITS):
        flips = jnp.where(distance == 1 << k, fields[6 + k], flips)
    row_flips[0] = flips.astype(jnp.bfloat16)
    row_flips[1] = (flips - flips.astype(jnp.bfloat16).astype(f32)).astype(jnp.bfloat16)
    flips = jnp.where(distance == LANES, fields[6 + SIDE_BITS], jnp.zeros((SIDE, SIDE), f32))
    for q in range(LANE_BITS):
        flips = jnp.where(distance == 1 << q, fields[q], flips)
    pair_flips[0] = flips.astype(jnp.bfloat16)
    pair_flips[1] = (flips - flips.astype(jnp.bfloat16).astype(f32)).astype(jnp.bfloat16)

    row_ids = lax.broadcasted_iota(jnp.int32, (SIDE, LANES), 0)
    lane_ids = lax.broadcasted_iota(jnp.int32, (SIDE, LANES), 1)
    inner_bits = [lane_ids >> q & 1 for q in range(LANE_BITS)]
    inner_bits += [row_ids >> k & 1 for k in range(1, SIDE_BITS)]
    inner_count = len(inner_bits)
    inner_energy = jnp.zeros((SIDE, LANES), f32)
    inner_ones = jnp.zeros((SIDE, LANES), jnp.int32)
    for q in range(inner_count):
        inner_ones = inner_ones + inner_bits[q]
        if q + 1 < inner_count:
            inner_energy = inner_energy + couplings[q] * (spin(inner_bits[q]) * spin(inner_bits[q + 1]))
    table[0] = inner_energy
    table[1] = inner_ones.astype(f32) * (1.0 / spins)

    chunk_qubits = row_bits - chunk_bits
    top_spin = spin(core)
    low_spins = [spin(bit_of(low, b)) for b in range(bits)]

    def fill(k, carry):
        ids = [bit_of(k, t) for t in range(chunk_qubits)]
        z = [spin(b) for b in ids]
        count = ids[0]
        for b in ids[1:]:
            count = count + b
        energy = f32(0.0)
        for t in range(chunk_qubits - 1):
            energy = energy + couplings[inner_count + 1 + t] * (z[t] * z[t + 1])
        edge[k] = couplings[inner_count] * z[0]
        for j in range(blocks):
            zb = [low_spins[b] * (-1.0 if j >> b & 1 else 1.0) for b in range(bits)] + [top_spin]
            ones_j = count + core
            for b in range(bits):
                ones_j = ones_j + (1 - bit_of(low, b) if j >> b & 1 else bit_of(low, b))
            e = energy + couplings[spins - 2 - bits] * (z[-1] * zb[0])
            for b in range(bits):
                e = e + couplings[spins - 1 - bits + b] * (zb[b] * zb[b + 1])
            outer_energy[j * chunks + k] = e
            outer_ones[j * chunks + k] = ones_j.astype(f32) * (1.0 / spins)
        return carry

    lax.fori_loop(0, chunks, fill, 0)

    sub = lax.broadcasted_iota(jnp.int32, (8, LANES), 0)
    imag = (sub & 1) == 1
    lane_edge = spin(lax.broadcasted_iota(jnp.int32, (8, LANES), 1) & 1) * (couplings[spins - 1] * top_spin)

    def start_sums(s, norm, tilt):
        sums[s, 0, :8] = norm
        sums[s, 0, 8:] = tilt
        for o in range(1, 2 * blocks):
            remote(
                sums.at[s, 0], sums.at[s, o], sum_send.at[s], sum_recv.at[s], sum_device(o)
            ).start()

    def finish_sums(s):
        others = sums.at[s, pl.ds(1, 2 * blocks - 1)]
        wait_bytes(others, sum_recv.at[s])
        wait_bytes(others, sum_send.at[s])
        total = sums[s, 0]
        for o in range(1, 2 * blocks):
            total = total + sums[s, o]
        norm = jnp.full((8, LANES), jnp.sum(total[:8]), f32)
        tilt = jnp.full((8, LANES), jnp.sum(total[8:]), f32)
        return norm, tilt

    zero = jnp.zeros((8, LANES), f32)

    def first_sums():
        def body(k, carry):
            norm, tilt = carry
            for side in range(2):
                base = pl.multiple_of(k * CHUNK + side * SIDE, SIDE)
                x = even[0, pl.ds(base, SIDE), :]
                w = x * x
                ones = table[1] + (outer_ones[k] + side / spins)
                norm = norm + jnp.sum(w.reshape(groups, 8, LANES), axis=0)
                tilt = tilt + jnp.sum((w * ones).reshape(groups, 8, LANES), axis=0)
            return norm, tilt

        return lax.fori_loop(0, chunks, body, (zero, zero))

    def step_values(s):
        norm, tilt = finish_sums(s)
        magnet = tilt / norm
        factor = jnp.sqrt(f32(rows * (LANES // 2) * 2 * blocks) / norm)
        half_root = jnp.sqrt(jnp.full((8, LANES), DT / 2.0, f32))
        root_kappa = jnp.sqrt(jnp.full((8, LANES), KAPPA, f32))
        first = kicks[pl.ds(2 * s, 1), :] * half_root
        second = kicks[pl.ds(2 * s + 1, 1), :] * half_root
        drift = root_kappa * magnet * DT
        marks[0, pl.ds(2 * s, 1), :] = (drift + first)[:1]
        marks[0, pl.ds(2 * s + 1, 1), :] = (drift + second)[:1]
        ratio = root_kappa * second * (1.0 / DT)
        damp = factor * (DT * KAPPA * 0.5)
        table[2] = table[0] + (ratio.reshape(1, 8, LANES) * table[1].reshape(groups, 8, LANES)).reshape(SIDE, LANES)
        rate = factor * DT
        return dict(
            magnet=magnet, factor=factor, kick=factor * root_kappa * first, damp=damp, ratio=ratio,
            rate=jnp.where(imag, -rate, rate),
        )

    def flip_tile(src, j, k):
        x = jnp.concatenate(
            [bufs[src][j, pl.ds(pl.multiple_of(k * CHUNK + side * SIDE, SIDE), SIDE), :] for side in range(2)],
            axis=1,
        )
        coarse = x.astype(jnp.bfloat16)
        fine = (x - coarse.astype(f32)).astype(jnp.bfloat16)
        left = jnp.concatenate([row_flips[0], row_flips[0], row_flips[1], coarse, fine, coarse], axis=1)
        right = jnp.concatenate([coarse, fine, coarse, pair_flips[0], pair_flips[0], pair_flips[1]], axis=0)
        return jnp.dot(left, right, preferred_element_type=f32)

    base_ones = table[1, :8]

    def finish(src, j, k, tile, values, carry):
        here, there = bufs[src], bufs[1 - src]
        ones = outer_ones[j * chunks + k]
        keeps = []
        for n in range(SIDE_BITS - 1):
            shift = base_ones + (ones + n / spins - values["magnet"])
            keeps.append(values["factor"] + shift * (values["kick"] - values["damp"] * shift))
        level = lane_edge + outer_energy[j * chunks + k]
        weights = [None] * (SIDE_BITS - 1)
        for side in range(2):
            shift = ones + side / spins - values["magnet"]
            base_level = level + values["ratio"] * shift + (-edge[k] if side else edge[k])
            link = -couplings[inner_count - 1] if side else couplings[inner_count - 1]
            for part in range(SIDE // PART):
                offset = k * CHUNK + side * SIDE + part * PART
                rows_here = pl.ds(pl.multiple_of(offset, PART), PART)
                x = here[j, rows_here, :]
                total = tile[part * PART : (part + 1) * PART, side * LANES : (side + 1) * LANES]
                for t in range(chunk_bits, row_bits):
                    moved = flip_bit(k, t - chunk_bits) * CHUNK + side * SIDE + part * PART
                    total = total + fields[6 + t] * here[j, pl.ds(pl.multiple_of(moved, PART), PART), :]
                for b in range(bits):
                    total = total + fields[6 + row_bits + b] * here[other_block(j, b), rows_here, :]
                total = total + fields[spins - 1] * far[j, rows_here, :]
                top = part * PART * 2 // SIDE
                side_level = base_level - link if top else base_level + link
                x3 = x.reshape(part_groups, 8, LANES)
                diagonal = table[2, part * PART : (part + 1) * PART].reshape(part_groups, 8, LANES) + side_level[None]
                turned = values["rate"] * (total.reshape(part_groups, 8, LANES) + x3 * diagonal)
                turned = jnp.where(imag[None], pltpu.roll(turned, 1, 1), pltpu.roll(turned, 7, 1))
                counts = [ones_in(part * part_groups + g) + side for g in range(part_groups)]
                keep = jnp.concatenate([keeps[n][None] for n in counts], axis=0)
                new = keep * x3 + turned
                there[j, rows_here, :] = new.reshape(PART, LANES)
                if carry is not None:
                    w = new * new
                    for g, n in enumerate(counts):
                        weights[n] = w[g] if weights[n] is None else weights[n] + w[g]
        if carry is None:
            return None
        norm, tilt = carry
        some, scaled = weights[0], None
        for n in range(1, SIDE_BITS - 1):
            some = some + weights[n]
            scaled = weights[n] * (n / spins) if scaled is None else scaled + weights[n] * (n / spins)
        return norm + some, tilt + scaled + (base_ones + ones) * some

    def update(src, j, begin, end, values, sums_too, carry=None):
        ahead[...] = flip_tile(src, j, begin)

        def body(m, carry):
            k = begin + 2 * m
            later[...] = flip_tile(src, j, k + 1)
            carry = finish(src, j, k, ahead, values, carry)
            ahead[...] = flip_tile(src, j, jnp.minimum(k + 2, end - 1))
            return finish(src, j, k + 1, later, values, carry)

        trips = lax.div(end - begin, 2)
        if not sums_too:
            def plain(m, nothing):
                body(m, None)
                return nothing

            lax.fori_loop(0, trips, plain, 0)
            return None
        return lax.fori_loop(0, trips, body, carry or (zero, zero))

    everything = pl.ds(0, rows)

    def far_ready(j):
        wait_bytes(far.at[j, everything], far_recv.at[j])

    def send_far(src, j, where=None):
        where = pl.ds(0, rows) if where is None else where
        remote(
            bufs[src].at[j, where], far.at[j, where], far_send.at[j], far_recv.at[j], core_device
        ).start()

    def send_next(src, j):
        pl.semaphore_wait(free.at[j], 1)
        wait_bytes(bufs[src].at[j], far_send.at[j])
        send_far(src, j)

    def release(j):
        pl.semaphore_signal(free.at[j], 1, device_id=core_device, device_id_type=MESH)

    def needed(s):
        return [j for j in range(blocks) if ones_in(j) <= steps - 1 - s]

    def is_needed(j, s):
        count = bit_of(j, 0)
        for b in range(1, bits):
            count = count + bit_of(j, b)
        return count <= steps - 1 - s

    order = sorted(range(blocks), key=lambda j: (ones_in(j), j))
    levels = [[j for j in order if ones_in(j) == n] for n in range(bits + 1)]

    def last_hop(j, p):
        on = [b for b in range(bits) if j >> b & 1]
        return on[-1] if 4 * p >= 3 * PIECES else on[p % (len(on) - 1)]

    def arrived(j, p):
        wait_bytes(even.at[j, rows_of(p)], arrive.at[j, p])
        send_far(0, j, rows_of(p))
        for b in range(bits):
            target = j | 1 << b
            if not j >> b & 1 and last_hop(target, p) == b:
                remote(
                    even.at[j, rows_of(p)], even.at[target, rows_of(p)],
                    relay_send.at[target], arrive.at[target, p], bit_device(b),
                ).start()

    def push(b, p):
        remote(
            even.at[0, rows_of(p)], even.at[1 << b, rows_of(p)],
            push_send.at[b], arrive.at[1 << b, p], bit_device(b),
        ).start()

    crossed = bit_of(low, bits - 1) != high
    for p in range(PIECES):
        wait_bytes(even.at[0, rows_of(p)], own_sem.at[p])
        for b in range(bits - 1):
            push(b, p)
        pl.when(away | jnp.logical_not(crossed))(functools.partial(push, bits - 1, p))
        send_far(0, 0, rows_of(p))
    start_sums(0, *first_sums())
    far_ready(0)

    @pl.when(home & crossed)
    def _():
        for p in range(PIECES):
            push(bits - 1, p)

    for j in reversed(levels[1]):
        for p in range(PIECES):
            arrived(j, p)
    wait_bytes(kicks, noise_sem)

    values = step_values(0)
    def whole(src, j, sums_too):
        far_ready(j)
        return update(src, j, 0, chunks, values, sums_too)

    start_sums(1, *update(0, 0, 0, chunks, values, True))
    release(0)
    for n in range(2, bits + 1):
        for j in levels[n - 2]:
            if j:
                whole(0, j, False)
                release(j)
                send_next(1, j)
        if n < bits:
            for p in range(PIECES):
                for j in levels[n]:
                    arrived(j, p)
    last = blocks - 1

    def late_block(t, carry):
        final = t == 2 * bits
        half = lax.div(t, bits)

        @pl.when((lax.rem(t, bits) == 0) & (t < 2 * bits))
        def _():
            def take(p, nothing):
                arrived(last, half * (PIECES // 2) + p)
                return nothing

            lax.fori_loop(0, PIECES // 2, take, 0)

        j = last - jnp.where(final, 0, lax.shift_left(1, lax.rem(t, bits)))

        @pl.when((t < bits) | final)
        def _():
            far_ready(j)

        begin = jnp.where(final, 0, half * (chunks // 2))
        end = jnp.where(final, chunks, (half + 1) * (chunks // 2))
        update(0, j, begin, end, values, False)

        @pl.when((t >= bits) & is_needed(j, 1))
        def _():
            release(j)

        @pl.when(t == 0)
        def _():
            send_next(1, 0)

        @pl.when((t > bits) & is_needed(last - 1, 1))
        def _():
            send_next(1, last - lax.shift_left(1, lax.rem(t - 1, bits)))

        return carry

    lax.fori_loop(0, 2 * bits + 1, late_block, 0)
    if last in needed(1):
        send_next(1, last)

    @pl.when(away)
    def _():
        wait_bytes(state, swap_send)
        wait_bytes(noise, noise_send)

    for b in range(bits):
        wait_bytes(even.at[0], push_send.at[b])
    for j in order:
        if ones_in(j) >= 2:
            wait_bytes(even.at[j], relay_send.at[j])

    for s in range(1, steps - 1):
        src = s % 2
        values = step_values(s)
        start_sums(s + 1, *whole(src, 0, True))
        release(0)
        previous = 0
        rest = needed(s)[1:]
        while rest:
            first = stop = rest[0]
            while stop in rest:
                stop += 1
            rest = [j for j in rest if j >= stop]

            def one_block(j, carry, first=first, previous=previous, src=src, s=s, values=values):
                far_ready(j)
                update(src, j, 0, chunks, values, False)

                @pl.when(is_needed(j, s + 1))
                def _():
                    release(j)

                before = jnp.where(j == first, previous, j - 1)

                @pl.when(is_needed(before, s + 1))
                def _():
                    send_next(1 - src, before)

                return carry

            lax.fori_loop(first, stop, one_block, 0)
            previous = stop - 1
        if previous in needed(s + 1):
            send_next(1 - src, previous)

    src = (steps - 1) % 2
    values = step_values(steps - 1)
    for o in range(1, 2 * paths):
        remote(marks.at[0], marks.at[o], mark_send, mark_recv, mark_device(o)).start()
    far_ready(0)

    def deliver(p):
        @pl.when(home)
        def _():
            pltpu.make_async_copy(bufs[1 - src].at[0, rows_of(p)], out.at[rows_of(p)], out_sem).start()

        @pl.when(away)
        def _():
            remote(
                bufs[1 - src].at[0, rows_of(p)], out.at[rows_of(p)], out_send, out_sem, swap_device
            ).start()

    def last_piece(p, carry):
        update(src, 0, p * piece_chunks, (p + 1) * piece_chunks, values, False)

        @pl.when(p > 0)
        def _():
            deliver(p - 1)

        return carry

    lax.fori_loop(0, PIECES, last_piece, 0)
    deliver(PIECES - 1)

    others = marks.at[pl.ds(1, 2 * paths - 1)]
    wait_bytes(others, mark_recv)
    wait_bytes(others, mark_send)
    total = marks[0]
    for o in range(1, 2 * paths):
        total = total + marks[o]
    record[...] = total
    for j in order:
        wait_bytes(even.at[j], far_send.at[j])
    wait_bytes(out, out_sem)

    @pl.when(away)
    def _():
        wait_bytes(out, out_send)


def shards(state, fields, couplings, noise):
    local_len = state.shape[2]
    steps = noise.shape[1]
    bits = lax.axis_size("gx").bit_length() - 2
    paths = lax.axis_size("gy") // 2
    spins = local_len.bit_length() - 1 + bits + 1
    blocks = 1 << bits
    rows = 2 * local_len // LANES
    chunks = rows // CHUNK
    f32 = jnp.float32
    mixed = state.reshape(2, rows // 2, LANES).transpose(1, 0, 2).reshape(rows, LANES)
    kicks = jnp.broadcast_to(noise.reshape(steps * 2, 1), (steps * 2, LANES))
    smem = pl.BlockSpec(memory_space=pltpu.SMEM)
    hbm = pl.BlockSpec(memory_space=pl.ANY)
    dma, regular = pltpu.SemaphoreType.DMA, pltpu.SemaphoreType.REGULAR
    tile = (steps * 2, LANES)
    out, record = pl.pallas_call(
        functools.partial(evolve_kernel, bits, paths, steps, spins),
        in_specs=[smem, smem, hbm, hbm],
        out_specs=[hbm, pl.BlockSpec(memory_space=pltpu.VMEM)],
        out_shape=[jax.ShapeDtypeStruct((rows, LANES), f32), jax.ShapeDtypeStruct(tile, f32)],
        scratch_shapes=[
            pltpu.VMEM((blocks, rows, LANES), f32),
            pltpu.VMEM((blocks, rows, LANES), f32),
            pltpu.VMEM((blocks, rows, LANES), f32),
            pltpu.VMEM((2, SIDE, SIDE), jnp.bfloat16),
            pltpu.VMEM((2, SIDE, SIDE), jnp.bfloat16),
            pltpu.VMEM((SIDE, SIDE), f32),
            pltpu.VMEM((SIDE, SIDE), f32),
            pltpu.VMEM((3, SIDE, LANES), f32),
            pltpu.SMEM((blocks * chunks,), f32),
            pltpu.SMEM((blocks * chunks,), f32),
            pltpu.SMEM((chunks,), f32),
            pltpu.VMEM((steps, 2 * blocks, 16, LANES), f32),
            pltpu.VMEM((2 * paths,) + tile, f32),
            pltpu.VMEM(tile, f32),
            dma((PIECES,)), dma, dma, dma, dma((blocks, PIECES)), dma((bits,)), dma((blocks,)),
            dma((blocks,)), dma((blocks,)), dma((steps,)), dma((steps,)), dma, dma, dma, dma,
            regular((blocks,)),
        ],
        compiler_params=pltpu.CompilerParams(has_side_effects=True, vmem_limit_bytes=60 << 20),
    )(fields, couplings, kicks, mixed)
    final = out.reshape(rows // 2, 2, LANES).transpose(1, 0, 2).reshape(1, 2, local_len)
    return final, record[:, 0].reshape(steps, 2)


def solution(mesh):
    placed = (P("gy", None, "gx"), P(), P(), P("gy", None, None))
    return jax.shard_map(
        shards, mesh=mesh, in_specs=placed, out_specs=(P("gy", None, "gx"), P()), check_vma=False
    )
```

```python
import functools

import jax
import jax.numpy as jnp
from jax import lax
from jax.experimental import pallas as pl
from jax.experimental.pallas import tpu as pltpu
from jax.sharding import PartitionSpec as P

KAPPA = 4.0
DT = 0.05
LANES = 128
LANE_BITS = 7
SIDE = 256
SIDE_BITS = 8
CHUNK = 2 * SIDE
PART = 64
PIECES = 16
QUARTERS = 4
DELIVERIES = 8
MESH = pl.DeviceIdType.MESH


def ones_in(value):
    return bin(value).count("1")


def bit_of(value, k):
    return lax.rem(lax.div(value, 1 << k), 2)


def flip_bit(value, k):
    return value + (1 - 2 * bit_of(value, k)) * (1 << k)


def flip_bits(value, mask):
    k = 0
    while mask >> k:
        if mask >> k & 1:
            value = flip_bit(value, k)
        k += 1
    return value


def other_block(j, b):
    return j ^ 1 << b if isinstance(j, int) else flip_bit(j, b)


def spin(bit):
    return (1 - 2 * bit).astype(jnp.float32)


def wait_bytes(ref, sem):
    pltpu.make_async_copy(ref, ref, sem).wait()


def evolve_kernel(
    bits, paths, steps, spins,
    fields, couplings, noise, state, out, record,
    even, odd, far, row_flips, pair_flips, near_parts, next_parts, ahead, later, table, outer_energy, outer_ones, edge, sums, marks, kicks,
    own_sem, swap_send, noise_sem, noise_send, arrive, push_send, relay_send,
    far_send, far_recv, sum_send, sum_recv, mark_send, mark_recv, out_sem, out_send, free,
):
    f32 = jnp.float32
    blocks = 1 << bits
    rows = state.shape[0]
    row_bits = rows.bit_length() - 1
    chunk_bits = CHUNK.bit_length() - 1
    bufs = (even, odd)
    chunks = rows // CHUNK
    piece = rows // PIECES
    delivery = rows // DELIVERIES
    delivery_chunks = delivery // CHUNK
    groups = SIDE // 8
    part_groups = PART // 8

    gx, gy = lax.axis_index("gx"), lax.axis_index("gy")
    high, low = lax.div(gx, blocks), lax.rem(gx, blocks)
    path, core = lax.div(gy, 2), lax.rem(gy, 2)
    home = high == core
    away = high != core
    swap_device = {"gx": core * blocks + low, "gy": path * 2 + high}
    core_device = {"gx": gx, "gy": path * 2 + 1 - core}

    def bit_device(b):
        return {"gx": high * blocks + flip_bit(low, b), "gy": gy}

    def sum_device(o):
        c = 1 - core if o >> bits & 1 else core
        return {"gx": high * blocks + flip_bits(low, o % blocks), "gy": path * 2 + c}

    def mark_device(o):
        h = 1 - high if o & 1 else high
        return {"gx": h * blocks + low, "gy": lax.rem(path + (o >> 1), paths) * 2 + core}

    def remote(src, dst, send, recv, device):
        return pltpu.make_async_remote_copy(
            src_ref=src, dst_ref=dst, send_sem=send, recv_sem=recv, device_id=device, device_id_type=MESH
        )

    def rows_of(p):
        return pl.ds(p * piece if isinstance(p, int) else pl.multiple_of(p * piece, piece), piece)

    def delivery_of(p):
        return pl.ds(p * delivery if isinstance(p, int) else pl.multiple_of(p * delivery, delivery), delivery)

    @pl.when(home)
    def _():
        for p in range(PIECES):
            pltpu.make_async_copy(state.at[rows_of(p)], even.at[0, rows_of(p)], own_sem.at[p]).start()
        pltpu.make_async_copy(noise, kicks, noise_sem).start()

    @pl.when(away)
    def _():
        remote(noise, kicks, noise_send, noise_sem, swap_device).start()
        for p in range(PIECES):
            remote(
                state.at[rows_of(p)], even.at[0, rows_of(p)], swap_send, own_sem.at[p], swap_device
            ).start()

    place_a = lax.broadcasted_iota(jnp.int32, (SIDE, SIDE), 0)
    place_b = lax.broadcasted_iota(jnp.int32, (SIDE, SIDE), 1)
    distance = place_a ^ place_b
    flips = jnp.zeros((SIDE, SIDE), f32)
    for k in range(1, SIDE_BITS):
        flips = jnp.where(distance == 1 << k, fields[6 + k], flips)
    row_flips[0] = flips.astype(jnp.bfloat16)
    row_flips[1] = (flips - flips.astype(jnp.bfloat16).astype(f32)).astype(jnp.bfloat16)
    flips = jnp.where(distance == LANES, fields[6 + SIDE_BITS], jnp.zeros((SIDE, SIDE), f32))
    for q in range(LANE_BITS):
        flips = jnp.where(distance == 1 << q, fields[q], flips)
    pair_flips[0] = flips.astype(jnp.bfloat16)
    pair_flips[1] = (flips - flips.astype(jnp.bfloat16).astype(f32)).astype(jnp.bfloat16)

    row_ids = lax.broadcasted_iota(jnp.int32, (SIDE, LANES), 0)
    lane_ids = lax.broadcasted_iota(jnp.int32, (SIDE, LANES), 1)
    inner_bits = [lane_ids >> q & 1 for q in range(LANE_BITS)]
    inner_bits += [row_ids >> k & 1 for k in range(1, SIDE_BITS)]
    inner_count = len(inner_bits)
    inner_energy = jnp.zeros((SIDE, LANES), f32)
    inner_ones = jnp.zeros((SIDE, LANES), jnp.int32)
    for q in range(inner_count):
        inner_ones = inner_ones + inner_bits[q]
        if q + 1 < inner_count:
            inner_energy = inner_energy + couplings[q] * (spin(inner_bits[q]) * spin(inner_bits[q + 1]))
    table[0] = inner_energy
    table[1] = inner_ones.astype(f32) * (1.0 / spins)

    chunk_qubits = row_bits - chunk_bits
    top_spin = spin(core)
    low_spins = [spin(bit_of(low, b)) for b in range(bits)]

    def fill(k, carry):
        ids = [bit_of(k, t) for t in range(chunk_qubits)]
        z = [spin(b) for b in ids]
        count = ids[0]
        for b in ids[1:]:
            count = count + b
        energy = f32(0.0)
        for t in range(chunk_qubits - 1):
            energy = energy + couplings[inner_count + 1 + t] * (z[t] * z[t + 1])
        edge[k] = couplings[inner_count] * z[0]
        for j in range(blocks):
            zb = [low_spins[b] * (-1.0 if j >> b & 1 else 1.0) for b in range(bits)] + [top_spin]
            ones_j = count + core
            for b in range(bits):
                ones_j = ones_j + (1 - bit_of(low, b) if j >> b & 1 else bit_of(low, b))
            e = energy + couplings[spins - 2 - bits] * (z[-1] * zb[0])
            for b in range(bits):
                e = e + couplings[spins - 1 - bits + b] * (zb[b] * zb[b + 1])
            outer_energy[j * chunks + k] = e
            outer_ones[j * chunks + k] = ones_j.astype(f32) * (1.0 / spins)
        return carry

    lax.fori_loop(0, chunks, fill, 0)

    sub = lax.broadcasted_iota(jnp.int32, (8, LANES), 0)
    imag = (sub & 1) == 1
    lane_edge = spin(lax.broadcasted_iota(jnp.int32, (8, LANES), 1) & 1) * (couplings[spins - 1] * top_spin)

    def start_sums(s, norm, tilt):
        sums[s, 0, :8] = norm
        sums[s, 0, 8:] = tilt
        for o in range(1, 2 * blocks):
            remote(
                sums.at[s, 0], sums.at[s, o], sum_send.at[s], sum_recv.at[s], sum_device(o)
            ).start()

    def finish_sums(s):
        others = sums.at[s, pl.ds(1, 2 * blocks - 1)]
        wait_bytes(others, sum_recv.at[s])
        wait_bytes(others, sum_send.at[s])
        total = sums[s, 0]
        for o in range(1, 2 * blocks):
            total = total + sums[s, o]
        norm = jnp.full((8, LANES), jnp.sum(total[:8]), f32)
        tilt = jnp.full((8, LANES), jnp.sum(total[8:]), f32)
        return norm, tilt

    zero = jnp.zeros((8, LANES), f32)

    def first_sums():
        def body(k, carry):
            norm, tilt = carry
            for side in range(2):
                base = pl.multiple_of(k * CHUNK + side * SIDE, SIDE)
                x = even[0, pl.ds(base, SIDE), :]
                w = x * x
                ones = table[1] + (outer_ones[k] + side / spins)
                norm = norm + jnp.sum(w.reshape(groups, 8, LANES), axis=0)
                tilt = tilt + jnp.sum((w * ones).reshape(groups, 8, LANES), axis=0)
            return norm, tilt

        return lax.fori_loop(0, chunks, body, (zero, zero))

    def step_values(s):
        norm, tilt = finish_sums(s)
        magnet = tilt / norm
        factor = jnp.sqrt(f32(rows * (LANES // 2) * 2 * blocks) / norm)
        half_root = jnp.sqrt(jnp.full((8, LANES), DT / 2.0, f32))
        root_kappa = jnp.sqrt(jnp.full((8, LANES), KAPPA, f32))
        first = kicks[pl.ds(2 * s, 1), :] * half_root
        second = kicks[pl.ds(2 * s + 1, 1), :] * half_root
        drift = root_kappa * magnet * DT
        marks[0, pl.ds(2 * s, 1), :] = (drift + first)[:1]
        marks[0, pl.ds(2 * s + 1, 1), :] = (drift + second)[:1]
        ratio = root_kappa * second * (1.0 / DT)
        damp = factor * (DT * KAPPA * 0.5)
        table[2] = table[0] + (ratio.reshape(1, 8, LANES) * table[1].reshape(groups, 8, LANES)).reshape(SIDE, LANES)
        rate = factor * DT
        return dict(
            magnet=magnet, factor=factor, kick=factor * root_kappa * first, damp=damp, ratio=ratio,
            rate=jnp.where(imag, -rate, rate),
        )

    def split(src, j, k, parts):
        k = jnp.minimum(k, chunks - 1)
        for side in range(2):
            x = bufs[src][j, pl.ds(pl.multiple_of(k * CHUNK + side * SIDE, SIDE), SIDE), :]
            coarse = x.astype(jnp.bfloat16)
            parts[0, :, side * LANES : (side + 1) * LANES] = coarse
            parts[1, :, side * LANES : (side + 1) * LANES] = (x - coarse.astype(f32)).astype(jnp.bfloat16)

    def flip_tile(parts, held=None):
        left = [parts[0], parts[1], parts[0], row_flips[0], row_flips[0], row_flips[1]]
        right = [pair_flips[0], pair_flips[0], pair_flips[1], parts[0], parts[1], parts[0]]
        if held is not None:
            for i in range(1, len(right)):
                right[i] = jnp.concatenate([right[i][:16] + held[i - 1], right[i][16:]], axis=0)
        return jnp.dot(
            jnp.concatenate(left, axis=1), jnp.concatenate(right, axis=0), preferred_element_type=f32
        )

    def hold(new):
        zeros = jnp.minimum(jnp.abs(new), 0.0)
        zeros = jnp.concatenate([zeros, zeros], axis=0).astype(jnp.bfloat16)
        return jnp.concatenate([zeros, zeros], axis=1)

    base_ones = table[1, :8]

    def finish(src, j, k, tile, values, carry):
        here, there = bufs[src], bufs[1 - src]
        ones = outer_ones[j * chunks + k]
        keeps = []
        for n in range(SIDE_BITS - 1):
            shift = base_ones + (ones + n / spins - values["magnet"])
            keeps.append(values["factor"] + shift * (values["kick"] - values["damp"] * shift))
        level = lane_edge + outer_energy[j * chunks + k]
        weights = [None] * (SIDE_BITS - 1)
        held = []
        for side in range(2):
            shift = ones + side / spins - values["magnet"]
            base_level = level + values["ratio"] * shift + (-edge[k] if side else edge[k])
            link = -couplings[inner_count - 1] if side else couplings[inner_count - 1]
            for part in range(SIDE // PART):
                offset = k * CHUNK + side * SIDE + part * PART
                rows_here = pl.ds(pl.multiple_of(offset, PART), PART)
                x = here[j, rows_here, :]
                total = tile[part * PART : (part + 1) * PART, side * LANES : (side + 1) * LANES]
                for t in range(chunk_bits, row_bits):
                    moved = flip_bit(k, t - chunk_bits) * CHUNK + side * SIDE + part * PART
                    total = total + fields[6 + t] * here[j, pl.ds(pl.multiple_of(moved, PART), PART), :]
                for b in range(bits):
                    total = total + fields[6 + row_bits + b] * here[other_block(j, b), rows_here, :]
                total = total + fields[spins - 1] * far[j, rows_here, :]
                top = part * PART * 2 // SIDE
                side_level = base_level - link if top else base_level + link
                x3 = x.reshape(part_groups, 8, LANES)
                diagonal = table[2, part * PART : (part + 1) * PART].reshape(part_groups, 8, LANES) + side_level[None]
                turned = values["rate"] * (total.reshape(part_groups, 8, LANES) + x3 * diagonal)
                turned = jnp.where(imag[None], pltpu.roll(turned, 1, 1), pltpu.roll(turned, 7, 1))
                counts = [ones_in(part * part_groups + g) + side for g in range(part_groups)]
                keep = jnp.concatenate([keeps[n][None] for n in counts], axis=0)
                new = keep * x3 + turned
                there[j, rows_here, :] = new.reshape(PART, LANES)
                lowest = new[0]
                for g in range(1, part_groups):
                    lowest = jnp.minimum(lowest, new[g])
                held.append(hold(lowest))
                if carry is not None:
                    w = new * new
                    for g, n in enumerate(counts):
                        weights[n] = w[g] if weights[n] is None else weights[n] + w[g]
        if carry is None:
            return None, held
        norm, tilt = carry
        some, scaled = weights[0], None
        for n in range(1, SIDE_BITS - 1):
            some = some + weights[n]
            scaled = weights[n] * (n / spins) if scaled is None else scaled + weights[n] * (n / spins)
        return (norm + some, tilt + scaled + (base_ones + ones) * some), held

    def update(src, j, begin, end, values, sums_too, carry=None):
        split(src, j, begin, near_parts)
        split(src, j, begin + 1, next_parts)
        ahead[...] = flip_tile(near_parts)
        later[...] = flip_tile(next_parts)
        split(src, j, begin + 2, near_parts)
        split(src, j, begin + 3, next_parts)

        def body(m, carry):
            k = begin + 2 * m
            carry, held = finish(src, j, k, ahead, values, carry)
            ahead[...] = flip_tile(near_parts, held)
            split(src, j, k + 4, near_parts)
            carry, held = finish(src, j, k + 1, later, values, carry)
            later[...] = flip_tile(next_parts, held)
            split(src, j, k + 5, next_parts)
            return carry

        trips = lax.div(end - begin, 2)
        if not sums_too:
            def plain(m, nothing):
                body(m, None)
                return nothing

            lax.fori_loop(0, trips, plain, 0)
            return None
        return lax.fori_loop(0, trips, body, carry or (zero, zero))

    everything = pl.ds(0, rows)

    def far_ready(j):
        wait_bytes(far.at[j, everything], far_recv.at[j])

    def send_far(src, j, where=None):
        where = pl.ds(0, rows) if where is None else where
        remote(
            bufs[src].at[j, where], far.at[j, where], far_send.at[j], far_recv.at[j], core_device
        ).start()

    def send_next(src, j):
        pl.semaphore_wait(free.at[j], 1)
        wait_bytes(bufs[src].at[j], far_send.at[j])
        send_far(src, j)

    def release(j):
        pl.semaphore_signal(free.at[j], 1, device_id=core_device, device_id_type=MESH)

    def needed(s):
        return [j for j in range(blocks) if ones_in(j) <= steps - 1 - s]

    def is_needed(j, s):
        count = bit_of(j, 0)
        for b in range(1, bits):
            count = count + bit_of(j, b)
        return count <= steps - 1 - s

    order = sorted(range(blocks), key=lambda j: (ones_in(j), j))
    levels = [[j for j in order if ones_in(j) == n] for n in range(bits + 1)]

    def last_hop(j, p):
        on = [b for b in range(bits) if j >> b & 1]
        return on[-1] if 4 * p >= 3 * PIECES else on[p % (len(on) - 1)]

    def arrived(j, p):
        wait_bytes(even.at[j, rows_of(p)], arrive.at[j, p])
        send_far(0, j, rows_of(p))
        for b in range(bits):
            target = j | 1 << b
            if not j >> b & 1 and last_hop(target, p) == b:
                remote(
                    even.at[j, rows_of(p)], even.at[target, rows_of(p)],
                    relay_send.at[target], arrive.at[target, p], bit_device(b),
                ).start()

    def push(b, p):
        remote(
            even.at[0, rows_of(p)], even.at[1 << b, rows_of(p)],
            push_send.at[b], arrive.at[1 << b, p], bit_device(b),
        ).start()

    crossed = bit_of(low, bits - 1) != high
    for p in range(PIECES):
        wait_bytes(even.at[0, rows_of(p)], own_sem.at[p])
        for b in range(bits - 1):
            push(b, p)
        pl.when(away | jnp.logical_not(crossed))(functools.partial(push, bits - 1, p))
        send_far(0, 0, rows_of(p))
    start_sums(0, *first_sums())
    far_ready(0)

    @pl.when(home & crossed)
    def _():
        for p in range(PIECES):
            push(bits - 1, p)

    for j in reversed(levels[1]):
        for p in range(PIECES):
            arrived(j, p)
    wait_bytes(kicks, noise_sem)

    values = step_values(0)
    def whole(src, j, sums_too):
        far_ready(j)
        return update(src, j, 0, chunks, values, sums_too)

    start_sums(1, *update(0, 0, 0, chunks, values, True))
    release(0)
    for n in range(2, bits + 1):
        for j in levels[n - 2]:
            if j:
                whole(0, j, False)
                release(j)
                send_next(1, j)
        if n < bits:
            for p in range(PIECES):
                for j in levels[n]:
                    arrived(j, p)
    last = blocks - 1

    def late_block(t, carry):
        final = t == QUARTERS * bits
        quarter = lax.div(t, bits)

        @pl.when((lax.rem(t, bits) == 0) & (t < QUARTERS * bits))
        def _():
            def take(p, nothing):
                arrived(last, quarter * (PIECES // QUARTERS) + p)
                return nothing

            lax.fori_loop(0, PIECES // QUARTERS, take, 0)

        j = last - jnp.where(final, 0, lax.shift_left(1, lax.rem(t, bits)))

        @pl.when((t < bits) | final)
        def _():
            far_ready(j)

        begin = jnp.where(final, 0, quarter * (chunks // QUARTERS))
        end = jnp.where(final, chunks, (quarter + 1) * (chunks // QUARTERS))
        update(0, j, begin, end, values, False)

        @pl.when((t >= (QUARTERS - 1) * bits) & is_needed(j, 1))
        def _():
            release(j)

        @pl.when(t == 0)
        def _():
            send_next(1, 0)

        @pl.when((t > (QUARTERS - 1) * bits) & is_needed(last - 1, 1))
        def _():
            send_next(1, last - lax.shift_left(1, lax.rem(t - 1, bits)))

        return carry

    lax.fori_loop(0, QUARTERS * bits + 1, late_block, 0)
    if last in needed(1):
        send_next(1, last)

    @pl.when(away)
    def _():
        wait_bytes(state, swap_send)
        wait_bytes(noise, noise_send)

    for b in range(bits):
        wait_bytes(even.at[0], push_send.at[b])
    for j in order:
        if ones_in(j) >= 2:
            wait_bytes(even.at[j], relay_send.at[j])

    for s in range(1, steps - 1):
        src = s % 2
        values = step_values(s)
        start_sums(s + 1, *whole(src, 0, True))
        release(0)
        previous = 0
        rest = needed(s)[1:]
        while rest:
            first = stop = rest[0]
            while stop in rest:
                stop += 1
            rest = [j for j in rest if j >= stop]

            def one_block(j, carry, first=first, previous=previous, src=src, s=s, values=values):
                far_ready(j)
                update(src, j, 0, chunks, values, False)

                @pl.when(is_needed(j, s + 1))
                def _():
                    release(j)

                before = jnp.where(j == first, previous, j - 1)

                @pl.when(is_needed(before, s + 1))
                def _():
                    send_next(1 - src, before)

                return carry

            lax.fori_loop(first, stop, one_block, 0)
            previous = stop - 1
        if previous in needed(s + 1):
            send_next(1 - src, previous)

    src = (steps - 1) % 2
    values = step_values(steps - 1)
    for o in range(1, 2 * paths):
        remote(marks.at[0], marks.at[o], mark_send, mark_recv, mark_device(o)).start()
    far_ready(0)

    def deliver(p):
        @pl.when(home)
        def _():
            pltpu.make_async_copy(bufs[1 - src].at[0, delivery_of(p)], out.at[delivery_of(p)], out_sem).start()

        @pl.when(away)
        def _():
            remote(
                bufs[1 - src].at[0, delivery_of(p)], out.at[delivery_of(p)], out_send, out_sem, swap_device
            ).start()

    def last_piece(p, carry):
        update(src, 0, p * delivery_chunks, (p + 1) * delivery_chunks, values, False)

        @pl.when(p > 0)
        def _():
            deliver(p - 1)

        return carry

    lax.fori_loop(0, DELIVERIES, last_piece, 0)
    deliver(DELIVERIES - 1)

    others = marks.at[pl.ds(1, 2 * paths - 1)]
    wait_bytes(others, mark_recv)
    wait_bytes(others, mark_send)
    total = marks[0]
    for o in range(1, 2 * paths):
        total = total + marks[o]
    record[...] = total
    for j in order:
        wait_bytes(even.at[j], far_send.at[j])
    wait_bytes(out, out_sem)

    @pl.when(away)
    def _():
        wait_bytes(out, out_send)


def shards(state, fields, couplings, noise):
    local_len = state.shape[2]
    steps = noise.shape[1]
    bits = lax.axis_size("gx").bit_length() - 2
    paths = lax.axis_size("gy") // 2
    spins = local_len.bit_length() - 1 + bits + 1
    blocks = 1 << bits
    rows = 2 * local_len // LANES
    chunks = rows // CHUNK
    f32 = jnp.float32
    mixed = state.reshape(2, rows // 2, LANES).transpose(1, 0, 2).reshape(rows, LANES)
    kicks = jnp.broadcast_to(noise.reshape(steps * 2, 1), (steps * 2, LANES))
    smem = pl.BlockSpec(memory_space=pltpu.SMEM)
    hbm = pl.BlockSpec(memory_space=pl.ANY)
    dma, regular = pltpu.SemaphoreType.DMA, pltpu.SemaphoreType.REGULAR
    tile = (steps * 2, LANES)
    out, record = pl.pallas_call(
        functools.partial(evolve_kernel, bits, paths, steps, spins),
        in_specs=[smem, smem, hbm, hbm],
        out_specs=[hbm, pl.BlockSpec(memory_space=pltpu.VMEM)],
        out_shape=[jax.ShapeDtypeStruct((rows, LANES), f32), jax.ShapeDtypeStruct(tile, f32)],
        scratch_shapes=[
            pltpu.VMEM((blocks, rows, LANES), f32),
            pltpu.VMEM((blocks, rows, LANES), f32),
            pltpu.VMEM((blocks, rows, LANES), f32),
            pltpu.VMEM((2, SIDE, SIDE), jnp.bfloat16),
            pltpu.VMEM((2, SIDE, SIDE), jnp.bfloat16),
            pltpu.VMEM((2, SIDE, SIDE), jnp.bfloat16),
            pltpu.VMEM((2, SIDE, SIDE), jnp.bfloat16),
            pltpu.VMEM((SIDE, SIDE), f32),
            pltpu.VMEM((SIDE, SIDE), f32),
            pltpu.VMEM((3, SIDE, LANES), f32),
            pltpu.SMEM((blocks * chunks,), f32),
            pltpu.SMEM((blocks * chunks,), f32),
            pltpu.SMEM((chunks,), f32),
            pltpu.VMEM((steps, 2 * blocks, 16, LANES), f32),
            pltpu.VMEM((2 * paths,) + tile, f32),
            pltpu.VMEM(tile, f32),
            dma((PIECES,)), dma, dma, dma, dma((blocks, PIECES)), dma((bits,)), dma((blocks,)),
            dma((blocks,)), dma((blocks,)), dma((steps,)), dma((steps,)), dma, dma, dma, dma,
            regular((blocks,)),
        ],
        compiler_params=pltpu.CompilerParams(has_side_effects=True, vmem_limit_bytes=60 << 20),
    )(fields, couplings, kicks, mixed)
    final = out.reshape(rows // 2, 2, LANES).transpose(1, 0, 2).reshape(1, 2, local_len)
    return final, record[:, 0].reshape(steps, 2)


def solution(mesh):
    placed = (P("gy", None, "gx"), P(), P(), P("gy", None, None))
    return jax.shard_map(
        shards, mesh=mesh, in_specs=placed, out_specs=(P("gy", None, "gx"), P()), check_vma=False
    )
```
